32 devices in a mesh: layer: 2 (over core), row: 4 (over y, x), col: 4 (over z).
Axes of the slice: x: 2, y: 2, z: 4, core: 2. Of those that a mesh axis runs over, the one named last changes fastest.
Arguments:
- root_rhs: float32 [32, 8, 1024], P(None, None, 'row'), may hold values from -6 to 6
- child_rhs: float32 [2, 32, 8, 1024], P('layer', None, None, 'row'), may hold values from -6 to 6
- root_factor: float32 [8, 8, 1024, 1024], P(None, None, 'row', 'col'), may hold values from -0.0625 to 0.0625
- child_factor: float32 [2, 8, 8, 1024, 1024], P('layer', None, None, 'row', 'col'), may hold values from -0.0625 to 0.0625
- coupling: float32 [2, 8, 8, 1024, 1024], P('layer', None, None, 'row', 'col'), may hold values from -0.0234375 to 0.0234375
- root_inverse: float32 [8, 1024, 1024], P(None, 'col', 'row'), as said below
- child_inverse: float32 [2, 8, 1024, 1024], P('layer', None, 'col', 'row'), as said below
Outputs:
- root_solution: float32 [32, 8, 1024], P(None, None, 'row')
- child_solution: float32 [2, 32, 8, 1024], P('layer', None, None, 'row')
The draws below stay inside these ranges and needn't reach their ends.
Inputs may be any that keep to these rules, and one draw needn't show every extreme that they name: Each block of root_inverse is lower triangular. Each block of child_inverse is lower triangular.
All inputs are finite; a program needn't handle non-finite values.
Results may differ from the reference program's by a relative error of at most 0.00015.
Values sent between devices are 32-bit elements; how exact they have to be, the bound alone decides.
No kernel may reach another device: no remote copies, remote signals or barrier semaphores. Data moves between devices by JAX's collectives and lax.ppermute only.
A program may use at most 128 MiB of HBM per device.

```python
import jax
import jax.numpy as jnp
from jax import lax

ROOT = 8192
CHILD = 8192
BLK = 1024
NRHS = 32
RB = 8
CB = 8


def lower_inverses(key, amount):
    off_key, diag_key = jax.random.split(key)
    lower_part = jax.random.normal(off_key, (amount, BLK, BLK), jnp.float32) * (0.5 / jnp.sqrt(BLK * 1.0))
    diagonal = jax.random.uniform(diag_key, (amount, BLK), jnp.float32, 0.5, 1.5)
    identity = jnp.eye(BLK, dtype=jnp.float32)
    return jnp.tril(lower_part, -1) + diagonal[:, :, None] * identity[None]


def draw_root_inverse(key, part):
    amount = ROOT // BLK
    return lower_inverses(jax.random.fold_in(key, 11), amount)


def draw_child_inverse(key, part):
    amount = CHILD // BLK
    return lower_inverses(jax.random.fold_in(key, 23), 2 * amount).reshape(2, amount, BLK, BLK)


def level_of(stream_key, shape, cuts, least, largest):
    loudness, own = 1.0, jax.random.fold_in(stream_key, 6)
    for axis_at, blocks in cuts:
        draws = jnp.exp(jax.random.uniform(jax.random.fold_in(own, axis_at), (blocks,), jnp.float32, least / len(cuts), largest / len(cuts)))
        loudness = loudness * jnp.repeat(draws, shape[axis_at] // blocks).reshape([-1 if axis == axis_at else 1 for axis in range(len(shape))])
    return loudness


def bell_draw(key, extent, spread, most, pieces=(), kind=jnp.bfloat16):
    level = level_of(key, extent, pieces, -0.22, 0.18) if pieces else 1.0
    result = jax.random.normal(key, extent, jnp.float32) * spread * level
    return jnp.minimum(jnp.maximum(result, -most), most).astype(kind)


def setup_inputs(seed: int = 0) -> dict:
    splits = jax.random.split(jax.random.key(seed), 8)
    root_rhs = bell_draw(splits[0], (NRHS, RB, BLK), 1.0, 6.0, ((2, 4),), jnp.float32)
    child_rhs = bell_draw(splits[1], (2, NRHS, CB, BLK), 1.0, 6.0, ((0, 2), (3, 4)), jnp.float32)
    root_factor = bell_draw(splits[2], (RB, RB, BLK, BLK), ((ROOT + CHILD) // 2) ** -0.5, 0.0625, ((2, 4), (3, 4)), jnp.float32)
    child_factor = bell_draw(splits[3], (2, CB, CB, BLK, BLK), ((ROOT + CHILD) // 2) ** -0.5, 0.0625, ((0, 2), (3, 4), (4, 4)), jnp.float32)
    coupling = bell_draw(splits[4], (2, RB, CB, BLK, BLK), (4 * (ROOT + CHILD)) ** -0.5, 0.0234375, ((0, 2), (3, 4), (4, 4)), jnp.float32)
    root_inverse = draw_root_inverse(jax.random.fold_in(splits[7], 71), 0)
    child_inverse = draw_child_inverse(jax.random.fold_in(splits[7], 71), 0)
    return {"root_rhs": root_rhs, "child_rhs": child_rhs, "root_factor": root_factor, "child_factor": child_factor, "coupling": coupling, "root_inverse": root_inverse, "child_inverse": child_inverse}


precise = lax.Precision.HIGHEST


def forward(factor, inverse, right, lifted):
    blocks = factor.shape[0]
    solved = jnp.zeros((blocks, right.shape[0], BLK), jnp.float32)
    for target in range(blocks):
        pending = right[:, target] - lifted[target]
        if target > 0:
            pending = pending - jnp.einsum("jnb,jab->na", solved[:target], factor[target, :target], precision=precise)
        solved = solved.at[target].set(jnp.einsum("nb,ab->na", pending, inverse[target], precision=precise))
    return solved


def backward(factor, inverse, values, lifted):
    blocks = factor.shape[0]
    solved = jnp.zeros((blocks, values.shape[1], BLK), jnp.float32)
    for target in reversed(range(blocks)):
        pending = values[target] - lifted[target]
        if target + 1 < blocks:
            pending = pending - jnp.einsum("ina,iab->nb", solved[target + 1:], factor[target + 1:, target], precision=precise)
        solved = solved.at[target].set(jnp.dot(pending, inverse[target], precision=precise))
    return solved


def reference(root_rhs, child_rhs, root_factor, child_factor, coupling, root_inverse, child_inverse):
    root_count = ROOT // BLK
    child_count = CHILD // BLK
    empty_child = jnp.zeros((child_count, NRHS, BLK), jnp.float32)
    child_forward = [forward(child_factor[layer], child_inverse[layer], child_rhs[layer], empty_child) for layer in range(2)]
    lifted = jnp.zeros((root_count, NRHS, BLK), jnp.float32)
    for layer in range(2):
        lifted = lifted + jnp.einsum("jnb,kjab->kna", child_forward[layer], coupling[layer], precision=precise)
    root_forward = forward(root_factor, root_inverse, root_rhs, lifted)
    root_solved = backward(root_factor, root_inverse, root_forward, jnp.zeros((root_count, NRHS, BLK), jnp.float32))
    child_outputs = []
    for layer in range(2):
        lowered = jnp.einsum("ina,ijab->jnb", root_solved, coupling[layer], precision=precise)
        child_solved = backward(child_factor[layer], child_inverse[layer], child_forward[layer], lowered)
        child_outputs.append(jnp.transpose(child_solved, (1, 0, 2)))
    root_solution = jnp.transpose(root_solved, (1, 0, 2))
    return root_solution, jnp.stack(child_outputs, 0)
```

```python
import jax
import jax.numpy as jnp
from jax import lax
from jax.sharding import PartitionSpec as P

precise = lax.Precision.HIGH


def sum_over(x, axis, size):
    if size > 4:
        return lax.psum(x, axis)
    total = x
    others = []
    for step in range(1, size):
        if size & (size - 1):
            pairs = [(at, (at + step) % size) for at in range(size)]
        else:
            pairs = [(at, at ^ step) for at in range(size)]
        others.append(lax.ppermute(x, axis, pairs))
    for other in others:
        total = total + other
    return total


def swap(x):
    return lax.ppermute(x, "layer", [(0, 1), (1, 0)])


def forward(factor, inverse, start, rows, cols, after):
    blocks = factor.shape[0]
    pending = [start[k] for k in range(blocks)]
    solved = []
    for k in range(blocks):
        residual = sum_over(pending[k], "col", cols)
        share = jnp.einsum("nb,ab->na", residual, inverse[k], precision=precise)
        value = sum_over(share, "row", rows)
        solved.append(value)
        if k + 1 < blocks:
            pending[k + 1] = pending[k + 1] - jnp.einsum(
                "na,ba->nb", value, factor[k + 1, k], precision=precise
            )
        if k + 2 < blocks:
            rest = jnp.einsum("na,mba->mnb", value, factor[k + 2 :, k], precision=precise)
            for m in range(k + 2, blocks):
                pending[m] = pending[m] - rest[m - k - 2]
        after(k, value)
    return solved


def backward(factor, inverse, start, rows, cols, after):
    blocks = factor.shape[0]
    pending = [start[k] for k in range(blocks)]
    solved = [None] * blocks
    for k in reversed(range(blocks)):
        residual = sum_over(pending[k], "row", rows)
        share = jnp.einsum("na,ab->nb", residual, inverse[k], precision=precise)
        value = sum_over(share, "col", cols)
        solved[k] = value
        if k > 0:
            pending[k - 1] = pending[k - 1] - jnp.einsum(
                "nb,ba->na", value, factor[k, k - 1], precision=precise
            )
        if k > 1:
            rest = jnp.einsum("nb,mba->mna", value, factor[k, : k - 1], precision=precise)
            for m in range(k - 1):
                pending[m] = pending[m] - rest[m]
        after(k, value)
    return solved


def make_local(layers, rows, cols):
    def local(root_rhs, child_rhs, root_factor, child_factor, coupling, root_inverse, child_inverse):
        first_row = lax.axis_index("row") == 0
        first_col = lax.axis_index("col") == 0
        layer = lax.axis_index("layer")
        columns = root_rhs.shape[0]
        half = columns // 2
        child_blocks = child_factor[0]
        child_inv = child_inverse[0]
        couple = coupling[0]
        child_count = child_blocks.shape[0]
        root_count = root_factor.shape[0]
        child_start = jnp.where(first_col, jnp.transpose(child_rhs[0], (1, 0, 2)), 0.0)
        lift = []

        def lift_part(j, value):
            lift.append(jnp.einsum("na,kba->knb", value, couple[:, j], precision=precise))

        child_forward = forward(child_blocks, child_inv, child_start, rows, cols, lift_part)
        lifted = lift[0]
        for part in lift[1:]:
            lifted = lifted + part
        mine = lax.dynamic_slice_in_dim(lifted, layer * half, half, 1)
        theirs = lax.dynamic_slice_in_dim(lifted, (1 - layer) * half, half, 1)
        lifted = mine + swap(theirs)
        right_half = lax.dynamic_slice_in_dim(root_rhs, layer * half, half, 0)
        root_start = jnp.where(first_col, jnp.transpose(right_half, (1, 0, 2)), 0.0) - lifted
        root_forward = forward(root_factor, root_inverse, root_start, rows, cols, lambda k, v: None)
        root_back = [jnp.where(first_row, v, 0.0) for v in root_forward]
        child_back = [jnp.where(first_row, v, 0.0) for v in child_forward]
        root_full = [None] * root_count

        def lower_part(i, value):
            other = swap(value)
            low = jnp.where(layer == 0, value, other)
            high = jnp.where(layer == 0, other, value)
            full = jnp.concatenate([low, high], 0)
            root_full[i] = full
            down = jnp.einsum("nb,kba->kna", full, couple[i], precision=precise)
            for k in range(child_count):
                child_back[k] = child_back[k] - down[k]

        backward(root_factor, root_inverse, root_back, rows, cols, lower_part)
        child_solved = backward(child_blocks, child_inv, child_back, rows, cols, lambda k, v: None)
        return jnp.stack(root_full, 1), jnp.stack(child_solved, 1)[None]

    return local


def solution(mesh):
    in_specs = (
        P(None, None, "row"),
        P("layer", None, None, "row"),
        P(None, None, "row", "col"),
        P("layer", None, None, "row", "col"),
        P("layer", None, None, "row", "col"),
        P(None, "col", "row"),
        P("layer", None, "col", "row"),
    )
    out_specs = (P(None, None, "row"), P("layer", None, None, "row"))
    local = make_local(mesh.shape["layer"], mesh.shape["row"], mesh.shape["col"])
    return jax.shard_map(local, mesh=mesh, in_specs=in_specs, out_specs=out_specs, check_vma=False)
```

```python
import jax
import jax.numpy as jnp
from jax import lax
from jax.experimental import pallas as pl
from jax.experimental.pallas import tpu as pltpu
from jax.sharding import PartitionSpec as P

precise = lax.Precision.HIGH


def sum_over(x, axis, size):
    if size > 4:
        return lax.psum(x, axis)
    total = x
    others = []
    for step in range(1, size):
        if size & (size - 1):
            pairs = [(at, (at + step) % size) for at in range(size)]
        else:
            pairs = [(at, at ^ step) for at in range(size)]
        others.append(lax.ppermute(x, axis, pairs))
    for other in others:
        total = total + other
    return total


def swap(x):
    return lax.ppermute(x, "layer", [(0, 1), (1, 0)])


def on_chip(factor, inverse):
    blocks, high, wide = factor.shape[0], factor.shape[2], factor.shape[3]

    def body(factor_ref, inverse_ref, beside_ref, kept_ref, sems):
        copies = [pltpu.make_async_copy(inverse_ref, kept_ref, sems.at[0])]
        for k in range(1, blocks):
            copies.append(pltpu.make_async_copy(factor_ref.at[k, k - 1], beside_ref.at[k - 1], sems.at[k]))
        for copy in copies:
            copy.start()
        for copy in copies:
            copy.wait()

    return pl.pallas_call(
        body,
        in_specs=[pl.BlockSpec(memory_space=pltpu.HBM)] * 2,
        out_specs=[pl.BlockSpec(memory_space=pltpu.VMEM)] * 2,
        out_shape=[
            jax.ShapeDtypeStruct((blocks - 1, high, wide), jnp.float32),
            jax.ShapeDtypeStruct(inverse.shape, jnp.float32),
        ],
        scratch_shapes=[pltpu.SemaphoreType.DMA((blocks,))],
        compiler_params=pltpu.CompilerParams(vmem_limit_bytes=1 << 20),
        name="on_chip",
    )(*[pltpu.with_memory_space_constraint(x, pltpu.HBM) for x in (factor, inverse)])


def mul(spec, x, tiles):
    return jnp.einsum(spec, x, tiles, precision=lax.Precision.HIGH)


def forward(factor, beside, inverse, start, rows, cols, after, first_known=None, during=None):
    blocks = inverse.shape[0]
    solved = []
    ahead = None
    for k in range(blocks):
        pending = start(k)
        if ahead is not None:
            pending = pending - ahead
        if k:
            pending = pending - mul("na,ba->nb", solved[k - 1], beside[k - 1])
        residual = first_known if (k == 0 and first_known is not None) else sum_over(pending, "col", cols)
        if during is not None:
            residual = during(k, residual)
        value = sum_over(mul("nb,ab->na", residual, inverse[k]), "row", rows)
        ahead = None
        if k and k + 1 < blocks:
            ahead = mul("jna,jba->nb", jnp.stack(solved, 0), factor[k + 1, :k])
        solved.append(value)
        after(k, value)
    return solved


def backward(factor, beside, inverse, start, rows, cols, after, first_known=None, during=None):
    blocks = inverse.shape[0]
    pending = [start(k) for k in range(blocks)]
    solved = [None] * blocks
    for k in reversed(range(blocks)):
        residual = first_known if (k == blocks - 1 and first_known is not None) else sum_over(pending[k], "row", rows)
        if during is not None:
            residual = during(k, residual)
        value = sum_over(mul("na,ab->nb", residual, inverse[k]), "col", cols)
        solved[k] = value
        if k > 0:
            pending[k - 1] = pending[k - 1] - mul("nb,ba->na", value, beside[k - 1])
        if k > 1:
            rest = mul("nb,mba->mna", value, factor[k, : k - 1])
            for m in range(k - 1):
                pending[m] = pending[m] - rest[m]
        after(k, value, pending)
    return solved


def make_local(layers, rows, cols):
    def local(root_rhs, child_rhs, root_factor, child_factor, coupling, root_inverse, child_inverse):
        first_row = lax.axis_index("row") == 0
        first_col = lax.axis_index("col") == 0
        layer = lax.axis_index("layer")
        columns = root_rhs.shape[0]
        half = columns // 2
        couple = coupling[0]
        child_count = child_factor.shape[1]
        root_count = root_factor.shape[0]
        child_tiles = on_chip(child_factor[0], child_inverse[0])
        root_tiles = []
        root_again = []
        child_again = []

        def ready(kept, at, factor, inverse):
            def during(k, residual):
                if k == at:
                    held = lax.optimization_barrier((factor, inverse, residual))
                    kept.extend(on_chip(held[0], held[1]))
                    residual = held[2]
                return residual

            return during

        root_ready = ready(root_tiles, child_count - 2, root_factor, root_inverse)
        again_ready = ready(root_again, root_count - 2, root_factor, root_inverse)
        child_ready = ready(child_again, 2, child_factor[0], child_inverse[0])
        child_own = child_rhs[0]
        child_forward = forward(
            child_factor[0],
            *child_tiles,
            lambda k: jnp.where(first_col, child_own[:, k], 0.0),
            rows,
            cols,
            lambda k, v: None,
            first_known=child_own[:, 0],
            during=root_ready,
        )
        stacked = jnp.stack(child_forward, 0)

        def lift(k, stacked):
            return jnp.einsum("jna,jba->nb", stacked, couple[k], precision=precise)

        def exchange(parts):
            mine = lax.dynamic_slice_in_dim(parts, layer * half, half, 1)
            theirs = lax.dynamic_slice_in_dim(parts, (1 - layer) * half, half, 1)
            return mine + swap(theirs)

        lifted = {0: exchange(lift(0, stacked)[None])[0]}

        def lift_next(k, residual):
            if k == 0 and root_count > 1:
                held, residual = lax.optimization_barrier((stacked, residual))
                lifted[1] = exchange(lift(1, held)[None])[0]
            elif k == 1 and root_count > 2:
                held, residual = lax.optimization_barrier((stacked, residual))
                parts = exchange(jnp.stack([lift(m, held) for m in range(2, min(4, root_count))], 0))
                for m in range(2, min(4, root_count)):
                    lifted[m] = parts[m - 2]
            elif k == 3 and root_count > 4:
                held, residual = lax.optimization_barrier((stacked, residual))
                parts = exchange(jnp.stack([lift(m, held) for m in range(4, root_count)], 0))
                for m in range(4, root_count):
                    lifted[m] = parts[m - 4]
            return again_ready(k, residual)

        right_half = lax.dynamic_slice_in_dim(root_rhs, layer * half, half, 0)
        root_forward = forward(
            root_factor,
            *root_tiles,
            lambda k: jnp.where(first_col, right_half[:, k], 0.0) - lifted[k],
            rows,
            cols,
            lambda k, v: None,
            during=lift_next,
        )
        child_back = [jnp.where(first_row, v, 0.0) for v in child_forward]
        root_full = [None] * root_count

        def lower_part(i, value, pending):
            other = swap(value)
            low = jnp.where(layer == 0, value, other)
            high = jnp.where(layer == 0, other, value)
            full = jnp.concatenate([low, high], 0)
            root_full[i] = full
            down = jnp.einsum("nb,kba->kna", full, couple[i], precision=precise)
            for k in range(child_count):
                child_back[k] = child_back[k] - down[k]

        backward(
            root_factor,
            *root_again,
            lambda k: jnp.where(first_row, root_forward[k], 0.0),
            rows,
            cols,
            lower_part,
            first_known=root_forward[root_count - 1],
            during=child_ready,
        )
        child_solved = backward(
            child_factor[0], *child_again, lambda k: child_back[k], rows, cols, lambda k, v, p: None
        )
        return jnp.stack(root_full, 1), jnp.stack(child_solved, 1)[None]

    return local


def solution(mesh):
    in_specs = (
        P(None, None, "row"),
        P("layer", None, None, "row"),
        P(None, None, "row", "col"),
        P("layer", None, None, "row", "col"),
        P("layer", None, None, "row", "col"),
        P(None, "col", "row"),
        P("layer", None, "col", "row"),
    )
    out_specs = (P(None, None, "row"), P("layer", None, None, "row"))
    local = make_local(mesh.shape["layer"], mesh.shape["row"], mesh.shape["col"])
    return jax.shard_map(local, mesh=mesh, in_specs=in_specs, out_specs=out_specs, check_vma=False)
```

```python
import jax
import jax.numpy as jnp
from jax import lax
from jax.experimental import pallas as pl
from jax.experimental.pallas import tpu as pltpu
from jax.sharding import PartitionSpec as P

precise = lax.Precision.HIGH


def parity(at):
    return at & 1


def partners(size):
    if size & (size - 1):
        return [[(at + step) % size for at in range(size)] for step in range(1, size)]
    steps = [1, 3, 2] if size == 4 else list(range(1, size))
    return [[at ^ step for at in range(size)] for step in steps]


def sum_over(x, axis, size, crossed=False):
    if size > 4:
        return lax.psum(x, axis)
    total = x
    others = []
    for goes in partners(size):
        if crossed:
            pairs = [
                (layer * size + at, (layer ^ parity(at) ^ parity(goes[at])) * size + goes[at])
                for layer in range(2)
                for at in range(size)
            ]
            others.append(lax.ppermute(x, ("layer", axis), pairs))
        else:
            others.append(lax.ppermute(x, axis, list(enumerate(goes))))
    for other in others:
        total = total + other
    return total


def swap(x):
    return lax.ppermute(x, "layer", [(0, 1), (1, 0)])


def on_chip(factor, inverse):
    blocks, high, wide = factor.shape[0], factor.shape[2], factor.shape[3]

    def body(factor_ref, inverse_ref, beside_ref, kept_ref, sems):
        copies = [pltpu.make_async_copy(inverse_ref, kept_ref, sems.at[0])]
        for k in range(1, blocks):
            copies.append(pltpu.make_async_copy(factor_ref.at[k, k - 1], beside_ref.at[k - 1], sems.at[k]))
        for copy in copies:
            copy.start()
        for copy in copies:
            copy.wait()

    return pl.pallas_call(
        body,
        in_specs=[pl.BlockSpec(memory_space=pltpu.HBM)] * 2,
        out_specs=[pl.BlockSpec(memory_space=pltpu.VMEM)] * 2,
        out_shape=[
            jax.ShapeDtypeStruct((blocks - 1, high, wide), jnp.float32),
            jax.ShapeDtypeStruct(inverse.shape, jnp.float32),
        ],
        scratch_shapes=[pltpu.SemaphoreType.DMA((blocks,))],
        compiler_params=pltpu.CompilerParams(vmem_limit_bytes=1 << 20),
        cost_estimate=priced(blocks),
        name="on_chip",
    )(*[pltpu.with_memory_space_constraint(x, pltpu.HBM) for x in (factor, inverse)])


def halves(x):
    high = x.astype(jnp.bfloat16)
    return high, (x - high.astype(jnp.float32)).astype(jnp.bfloat16)


def product(high, both, tile, dims):
    count = high.shape[0]
    th, tl = halves(tile)
    dot = lambda x, y: lax.dot_general(x, y, (dims, ((), ())), preferred_element_type=jnp.float32)
    main = dot(both, th)
    return main[:count] + (main[count:] + dot(high, tl))


def priced(tiles):
    return pl.CostEstimate(flops=250_000_000 * tiles, bytes_accessed=1 << 18, transcendentals=0)


def lift_kernel(stacked, couple, at):
    inner, columns, wide = stacked.shape
    high = couple.shape[2]
    chunk = inner // 2 if inner % 2 == 0 else inner

    def body(u_ref, p_ref, out_ref):
        step = pl.program_id(0)
        total = None
        for j in range(chunk):
            top, low = halves(u_ref[step * chunk + j])
            part = product(top, jnp.concatenate([top, low], 0), p_ref[0, j], ((1,), (1,)))
            total = part if total is None else total + part

        @pl.when(step == 0)
        def _():
            out_ref[0] = total

        @pl.when(step != 0)
        def _():
            out_ref[0] += total

    return pl.pallas_call(
        body,
        grid=(inner // chunk,),
        in_specs=[
            pl.BlockSpec((inner, columns, wide), lambda j: (0, 0, 0)),
            pl.BlockSpec((1, chunk, high, wide), lambda j: (at, j, 0, 0)),
        ],
        out_specs=pl.BlockSpec((1, columns, high), lambda j: (0, 0, 0)),
        out_shape=jax.ShapeDtypeStruct((1, columns, high), jnp.float32),
        compiler_params=pltpu.CompilerParams(vmem_limit_bytes=8 << 20),
        cost_estimate=priced(inner),
        name="lift",
    )(stacked, pltpu.with_memory_space_constraint(couple, pltpu.HBM))


def lower_kernel(value, couple, row, before):
    count, columns, wide = before.shape
    high = couple.shape[2]
    chunk = 4 if count % 4 == 0 else 1

    def body(s_ref, p_ref, before_ref, out_ref):
        top, low = halves(s_ref[...])
        both = jnp.concatenate([top, low], 0)
        for k in range(chunk):
            out_ref[k] = before_ref[k] - product(top, both, p_ref[0, k], ((1,), (0,)))

    return pl.pallas_call(
        body,
        grid=(count // chunk,),
        in_specs=[
            pl.BlockSpec((columns, high), lambda k: (0, 0)),
            pl.BlockSpec((1, chunk, high, wide), lambda k: (row, k, 0, 0)),
            pl.BlockSpec((chunk, columns, wide), lambda k: (k, 0, 0)),
        ],
        out_specs=pl.BlockSpec((chunk, columns, wide), lambda k: (k, 0, 0)),
        out_shape=jax.ShapeDtypeStruct(before.shape, jnp.float32),
        compiler_params=pltpu.CompilerParams(vmem_limit_bytes=8 << 20),
        cost_estimate=priced(count),
        name="lower",
    )(value, pltpu.with_memory_space_constraint(couple, pltpu.HBM), before)


def mul(spec, x, tiles):
    return jnp.einsum(spec, x, tiles, precision=lax.Precision.HIGH)


def forward(factor, beside, inverse, start, rows, cols, after, first_known=None, during=None, crossed=False):
    blocks = inverse.shape[0]
    solved = []
    ahead = None
    for k in range(blocks):
        pending = start(k)
        if ahead is not None:
            pending = pending - ahead
        if k:
            pending = pending - mul("na,ba->nb", solved[k - 1], beside[k - 1])
        residual = first_known if (k == 0 and first_known is not None) else sum_over(pending, "col", cols, crossed)
        if during is not None:
            residual = during(k, residual)
        value = sum_over(mul("nb,ab->na", residual, inverse[k]), "row", rows, crossed)
        ahead = None
        if k and k + 1 < blocks:
            ahead = mul("jna,jba->nb", jnp.stack(solved, 0), factor[k + 1, :k])
        solved.append(value)
        after(k, value)
    return solved


def backward(factor, beside, inverse, start, rows, cols, after, first_known=None, during=None, crossed=False):
    blocks = inverse.shape[0]
    pending = [start(k) for k in range(blocks)]
    solved = [None] * blocks
    for k in reversed(range(blocks)):
        residual = first_known if (k == blocks - 1 and first_known is not None) else sum_over(pending[k], "row", rows, crossed)
        if during is not None:
            residual = during(k, residual)
        value = sum_over(mul("na,ab->nb", residual, inverse[k]), "col", cols, crossed)
        solved[k] = value
        if k > 0:
            pending[k - 1] = pending[k - 1] - mul("nb,ba->na", value, beside[k - 1])
        if k > 1:
            rest = mul("nb,mba->mna", value, factor[k, : k - 1])
            for m in range(k - 1):
                pending[m] = pending[m] - rest[m]
        after(k, value, pending)
    return solved


def make_local(layers, rows, cols):
    def local(root_rhs, child_rhs, root_factor, child_factor, coupling, root_inverse, child_inverse):
        first_row = lax.axis_index("row") == 0
        first_col = lax.axis_index("col") == 0
        layer = lax.axis_index("layer")
        crossed = layers == 2 and rows <= 4 and cols <= 4
        side = layer
        if crossed:
            side = layer ^ parity(lax.axis_index("row")) ^ parity(lax.axis_index("col"))
        columns = root_rhs.shape[0]
        half = columns // 2
        couple = coupling[0]
        child_count = child_factor.shape[1]
        root_count = root_factor.shape[0]
        child_tiles = on_chip(child_factor[0], child_inverse[0])
        root_tiles = []
        root_again = []
        child_again = []

        def ready(kept, at, factor, inverse):
            def during(k, residual):
                if k == at:
                    held = lax.optimization_barrier((factor, inverse, residual))
                    kept.extend(on_chip(held[0], held[1]))
                    residual = held[2]
                return residual

            return during

        root_ready = ready(root_tiles, child_count - 2, root_factor, root_inverse)
        again_ready = ready(root_again, root_count - 2, root_factor, root_inverse)
        child_ready = ready(child_again, 2, child_factor[0], child_inverse[0])
        child_own = child_rhs[0]
        child_forward = forward(
            child_factor[0],
            *child_tiles,
            lambda k: jnp.where(first_col, child_own[:, k], 0.0),
            rows,
            cols,
            lambda k, v: None,
            first_known=child_own[:, 0],
            during=root_ready,
        )
        stacked = jnp.stack(child_forward, 0)

        def exchange(parts):
            mine = lax.dynamic_slice_in_dim(parts, side * half, half, 1)
            theirs = lax.dynamic_slice_in_dim(parts, (1 - side) * half, half, 1)
            return mine + swap(theirs)

        lifted = {0: exchange(lift_kernel(stacked, couple, 0))[0]}

        def lift_next(k, residual):
            if k + 1 < root_count:
                held, residual = lax.optimization_barrier((stacked, residual))
                lifted[k + 1] = exchange(lift_kernel(held, couple, k + 1))[0]
            return again_ready(k, residual)

        right_half = lax.dynamic_slice_in_dim(root_rhs, side * half, half, 0)
        root_forward = forward(
            root_factor,
            *root_tiles,
            lambda k: jnp.where(first_col, right_half[:, k], 0.0) - lifted[k],
            rows,
            cols,
            lambda k, v: None,
            during=lift_next,
            crossed=crossed,
        )
        child_back = [jnp.where(first_row, stacked, 0.0)]
        root_full = [None] * root_count

        def lower_part(i, value, pending):
            other = swap(value)
            low = jnp.where(side == 0, value, other)
            high = jnp.where(side == 0, other, value)
            full = jnp.concatenate([low, high], 0)
            root_full[i] = full
            child_back.append(lower_kernel(full, couple, i, child_back[-1]))

        backward(
            root_factor,
            *root_again,
            lambda k: jnp.where(first_row, root_forward[k], 0.0),
            rows,
            cols,
            lower_part,
            first_known=root_forward[root_count - 1],
            during=child_ready,
            crossed=crossed,
        )
        child_solved = backward(
            child_factor[0], *child_again, lambda k: child_back[-1][k], rows, cols, lambda k, v, p: None
        )
        return jnp.stack(root_full, 1), jnp.stack(child_solved, 1)[None]

    return local


def solution(mesh):
    in_specs = (
        P(None, None, "row"),
        P("layer", None, None, "row"),
        P(None, None, "row", "col"),
        P("layer", None, None, "row", "col"),
        P("layer", None, None, "row", "col"),
        P(None, "col", "row"),
        P("layer", None, "col", "row"),
    )
    out_specs = (P(None, None, "row"), P("layer", None, None, "row"))
    local = make_local(mesh.shape["layer"], mesh.shape["row"], mesh.shape["col"])
    return jax.shard_map(local, mesh=mesh, in_specs=in_specs, out_specs=out_specs, check_vma=False)
```

```python
import jax
import jax.numpy as jnp
from jax import lax
from jax.experimental import pallas as pl
from jax.experimental.pallas import tpu as pltpu
from jax.sharding import PartitionSpec as P

precise = lax.Precision.HIGH


def parity(at):
    return at & 1


def partners(size):
    if size & (size - 1):
        return [[(at + step) % size for at in range(size)] for step in range(1, size)]
    steps = [1, 3, 2] if size == 4 else list(range(1, size))
    return [[at ^ step for at in range(size)] for step in steps]


def sum_over(x, axis, size, crossed=False):
    if size > 4:
        return lax.psum(x, axis)
    total = x
    others = []
    for goes in partners(size):
        if crossed:
            pairs = [
                (layer * size + at, (layer ^ parity(at) ^ parity(goes[at])) * size + goes[at])
                for layer in range(2)
                for at in range(size)
            ]
            others.append(lax.ppermute(x, ("layer", axis), pairs))
        else:
            others.append(lax.ppermute(x, axis, list(enumerate(goes))))
    for other in others:
        total = total + other
    return total


def swap(x):
    return lax.ppermute(x, "layer", [(0, 1), (1, 0)])


def on_chip(factor, inverse):
    blocks, high, wide = factor.shape[0], factor.shape[2], factor.shape[3]

    def body(factor_ref, inverse_ref, *refs):
        kept_ref, beside_refs, sems = refs[0], refs[1:-1], refs[-1]
        copies = [pltpu.make_async_copy(inverse_ref, kept_ref, sems.at[0])]
        for k in range(1, blocks):
            copies.append(pltpu.make_async_copy(factor_ref.at[k, k - 1], beside_refs[k - 1], sems.at[k]))
        for copy in copies:
            copy.start()
        for copy in copies:
            copy.wait()

    kept, *beside = pl.pallas_call(
        body,
        in_specs=[pl.BlockSpec(memory_space=pltpu.HBM)] * 2,
        out_specs=[pl.BlockSpec(memory_space=pltpu.VMEM)] * blocks,
        out_shape=[jax.ShapeDtypeStruct(inverse.shape, jnp.float32)]
        + [jax.ShapeDtypeStruct((high, wide), jnp.float32)] * (blocks - 1),
        scratch_shapes=[pltpu.SemaphoreType.DMA((blocks,))],
        compiler_params=pltpu.CompilerParams(vmem_limit_bytes=1 << 20),
        cost_estimate=priced(blocks),
        name="on_chip",
    )(*[pltpu.with_memory_space_constraint(x, pltpu.HBM) for x in (factor, inverse)])
    return beside, kept


def halves(x):
    high = x.astype(jnp.bfloat16)
    return high, (x - high.astype(jnp.float32)).astype(jnp.bfloat16)


def product(high, both, tile, dims):
    count = high.shape[0]
    th, tl = halves(tile)
    dot = lambda x, y: lax.dot_general(x, y, (dims, ((), ())), preferred_element_type=jnp.float32)
    main = dot(both, th)
    return main[:count] + (main[count:] + dot(high, tl))


def priced(tiles):
    return pl.CostEstimate(flops=250_000_000 * tiles, bytes_accessed=1 << 18, transcendentals=0)


def lift_kernel(stacked, couple, at):
    inner, columns, wide = stacked.shape
    high = couple.shape[2]
    chunk = inner // 2 if inner % 2 == 0 else inner

    def body(u_ref, p_ref, out_ref):
        step = pl.program_id(0)
        total = None
        for j in range(chunk):
            top, low = halves(u_ref[step * chunk + j])
            part = product(top, jnp.concatenate([top, low], 0), p_ref[0, j], ((1,), (1,)))
            total = part if total is None else total + part

        @pl.when(step == 0)
        def _():
            out_ref[0] = total

        @pl.when(step != 0)
        def _():
            out_ref[0] += total

    return pl.pallas_call(
        body,
        grid=(inner // chunk,),
        in_specs=[
            pl.BlockSpec((inner, columns, wide), lambda j: (0, 0, 0)),
            pl.BlockSpec((1, chunk, high, wide), lambda j: (at, j, 0, 0)),
        ],
        out_specs=pl.BlockSpec((1, columns, high), lambda j: (0, 0, 0)),
        out_shape=jax.ShapeDtypeStruct((1, columns, high), jnp.float32),
        compiler_params=pltpu.CompilerParams(vmem_limit_bytes=8 << 20),
        cost_estimate=priced(inner),
        name="lift",
    )(stacked, pltpu.with_memory_space_constraint(couple, pltpu.HBM))


def lower_kernel(value, couple, row, before):
    count, columns, wide = before.shape
    high = couple.shape[2]
    chunk = 4 if count % 4 == 0 else 1

    def body(s_ref, p_ref, before_ref, out_ref):
        top, low = halves(s_ref[...])
        both = jnp.concatenate([top, low], 0)
        for k in range(chunk):
            out_ref[k] = before_ref[k] - product(top, both, p_ref[0, k], ((1,), (0,)))

    return pl.pallas_call(
        body,
        grid=(count // chunk,),
        in_specs=[
            pl.BlockSpec((columns, high), lambda k: (0, 0)),
            pl.BlockSpec((1, chunk, high, wide), lambda k: (row, k, 0, 0)),
            pl.BlockSpec((chunk, columns, wide), lambda k: (k, 0, 0)),
        ],
        out_specs=pl.BlockSpec((chunk, columns, wide), lambda k: (k, 0, 0)),
        out_shape=jax.ShapeDtypeStruct(before.shape, jnp.float32),
        compiler_params=pltpu.CompilerParams(vmem_limit_bytes=8 << 20),
        cost_estimate=priced(count),
        name="lower",
    )(value, pltpu.with_memory_space_constraint(couple, pltpu.HBM), before)


def mul(spec, x, tiles):
    return jnp.einsum(spec, x, tiles, precision=lax.Precision.HIGH)


def forward(factor, beside, inverse, start, rows, cols, after, first_known=None, during=None, crossed=False):
    blocks = inverse.shape[0]
    solved = []
    ahead = None
    for k in range(blocks):
        pending = start(k)
        if ahead is not None:
            pending = pending - ahead
        if k:
            pending = pending - mul("na,ba->nb", solved[k - 1], beside[k - 1])
        residual = first_known if (k == 0 and first_known is not None) else sum_over(pending, "col", cols, crossed)
        if during is not None:
            residual = during(k, residual)
        value = sum_over(mul("nb,ab->na", residual, inverse[k]), "row", rows, crossed)
        ahead = None
        if k and k + 1 < blocks:
            ahead = mul("jna,jba->nb", jnp.stack(solved, 0), factor[k + 1, :k])
        solved.append(value)
        after(k, value)
    return solved


def backward(factor, beside, inverse, start, rows, cols, after, first_known=None, during=None, crossed=False):
    blocks = inverse.shape[0]
    pending = [start(k) for k in range(blocks)]
    solved = [None] * blocks
    for k in reversed(range(blocks)):
        residual = first_known if (k == blocks - 1 and first_known is not None) else sum_over(pending[k], "row", rows, crossed)
        if during is not None:
            residual = during(k, residual)
        value = sum_over(mul("na,ab->nb", residual, inverse[k]), "col", cols, crossed)
        solved[k] = value
        if k > 0:
            pending[k - 1] = pending[k - 1] - mul("nb,ba->na", value, beside[k - 1])
        if k > 1:
            rest = mul("nb,mba->mna", value, factor[k, : k - 1])
            for m in range(k - 1):
                pending[m] = pending[m] - rest[m]
        after(k, value, pending)
    return solved


def make_local(layers, rows, cols):
    def local(root_rhs, child_rhs, root_factor, child_factor, coupling, root_inverse, child_inverse):
        first_row = lax.axis_index("row") == 0
        first_col = lax.axis_index("col") == 0
        layer = lax.axis_index("layer")
        crossed = layers == 2 and rows <= 4 and cols <= 4
        side = layer
        if crossed:
            side = layer ^ parity(lax.axis_index("row")) ^ parity(lax.axis_index("col"))
        columns = root_rhs.shape[0]
        half = columns // 2
        couple = coupling[0]
        child_count = child_factor.shape[1]
        root_count = root_factor.shape[0]
        child_tiles = on_chip(child_factor[0], child_inverse[0])
        root_tiles = []
        root_again = []
        child_again = []

        def ready(kept, at, factor, inverse):
            def during(k, residual):
                if k == at:
                    held = lax.optimization_barrier((factor, inverse, residual))
                    kept.extend(on_chip(held[0], held[1]))
                    residual = held[2]
                return residual

            return during

        root_ready = ready(root_tiles, child_count - 2, root_factor, root_inverse)
        again_ready = ready(root_again, root_count - 2, root_factor, root_inverse)
        child_ready = ready(child_again, 2, child_factor[0], child_inverse[0])
        child_own = child_rhs[0]
        child_forward = forward(
            child_factor[0],
            *child_tiles,
            lambda k: jnp.where(first_col, child_own[:, k], 0.0),
            rows,
            cols,
            lambda k, v: None,
            first_known=child_own[:, 0],
            during=root_ready,
        )
        stacked = jnp.stack(child_forward, 0)

        def exchange(parts):
            mine = lax.dynamic_slice_in_dim(parts, side * half, half, 1)
            theirs = lax.dynamic_slice_in_dim(parts, (1 - side) * half, half, 1)
            return mine + swap(theirs)

        lifted = {0: exchange(lift_kernel(stacked, couple, 0))[0]}

        def lift_next(k, residual):
            if k + 1 < root_count:
                held, residual = lax.optimization_barrier((stacked, residual))
                lifted[k + 1] = exchange(lift_kernel(held, couple, k + 1))[0]
            return again_ready(k, residual)

        right_half = lax.dynamic_slice_in_dim(root_rhs, side * half, half, 0)
        root_forward = forward(
            root_factor,
            *root_tiles,
            lambda k: jnp.where(first_col, right_half[:, k], 0.0) - lifted[k],
            rows,
            cols,
            lambda k, v: None,
            during=lift_next,
            crossed=crossed,
        )
        child_back = [jnp.where(first_row, stacked, 0.0)]
        root_full = [None] * root_count

        def lower_part(i, value, pending):
            other = swap(value)
            low = jnp.where(side == 0, value, other)
            high = jnp.where(side == 0, other, value)
            full = jnp.concatenate([low, high], 0)
            root_full[i] = full
            child_back.append(lower_kernel(full, couple, i, child_back[-1]))

        backward(
            root_factor,
            *root_again,
            lambda k: jnp.where(first_row, root_forward[k], 0.0),
            rows,
            cols,
            lower_part,
            first_known=root_forward[root_count - 1],
            during=child_ready,
            crossed=crossed,
        )
        child_solved = backward(
            child_factor[0], *child_again, lambda k: child_back[-1][k], rows, cols, lambda k, v, p: None
        )
        return jnp.stack(root_full, 1), jnp.stack(child_solved, 1)[None]

    return local


def solution(mesh):
    in_specs = (
        P(None, None, "row"),
        P("layer", None, None, "row"),
        P(None, None, "row", "col"),
        P("layer", None, None, "row", "col"),
        P("layer", None, None, "row", "col"),
        P(None, "col", "row"),
        P("layer", None, "col", "row"),
    )
    out_specs = (P(None, None, "row"), P("layer", None, None, "row"))
    local = make_local(mesh.shape["layer"], mesh.shape["row"], mesh.shape["col"])
    return jax.shard_map(local, mesh=mesh, in_specs=in_specs, out_specs=out_specs, check_vma=False)
```
